32 devices in a mesh: owner: 4 (over x, core), rows: 8 (over z, y).
Axes of the slice: x: 2, y: 2, z: 4, core: 2. Of those that a mesh axis runs over, the one named last changes fastest.
Arguments:
- train_gate: float32 [128, 2048, 768], P('owner', 'rows'), may hold values from -0.1875 to 0.1875
- train_up: float32 [128, 2048, 768], P('owner', 'rows'), may hold values from -0.1875 to 0.1875
- router_weight: float32 [2048, 128], P('rows', 'owner'), may hold values from -0.125 to 0.125
- router_gain: float32 [2048], P('rows'), may hold values from 0.25 to 1.75
Outputs:
- ready_gate: bfloat16 [128, 2048, 768], P(('owner', 'rows'))
- ready_up: bfloat16 [128, 2048, 768], P(('owner', 'rows'))
- scale_gate: float32 [128, 768], P(('owner', 'rows'))
- scale_up: float32 [128, 768], P(('owner', 'rows'))
- serve_router: bfloat16 [2048, 128], replicated
The draws below stay inside these ranges and needn't reach their ends.
All inputs are finite; a program needn't handle non-finite values.
Results may differ from the reference program's by a relative error of at most 0.001.
Values may be sent and summed in bfloat16 or wider, within the bound.
A program may use at most 192 MiB of HBM per device.

```python
import jax
import jax.numpy as jnp
from jax import lax

EXPERTS = 128
D_MODEL = 2048
D_EXPERT = 768


def spiked(drawn, rng, source, target, parts, factor):
    def block_of(position):
        return (jnp.arange(drawn.shape[position]) // (drawn.shape[position] // parts)).reshape((-1,) + (1,) * (drawn.ndim - 1 - position))

    near = jax.random.permutation(rng, parts)[block_of(target)]
    other_side = (block_of(target) + parts // 2) % parts
    return jnp.where((block_of(source) == near) | (block_of(source) == other_side), factor * drawn, drawn)


def shard_levels(key, dims, cuts, low, high):
    loudness, own = 1.0, jax.random.fold_in(key, 6)
    for axis_at, blocks in cuts:
        heights = jnp.exp(jax.random.uniform(jax.random.fold_in(own, axis_at), (blocks,), jnp.float32, low / len(cuts), high / len(cuts)))
        loudness = loudness * jnp.repeat(heights, dims[axis_at] // blocks).reshape([-1 if axis == axis_at else 1 for axis in range(len(dims))])
    return loudness


def noise(stream_key, extent, spread, most, split=(), dtype=jnp.bfloat16):
    result = jax.random.normal(stream_key, extent, jnp.float32) * spread
    if len(split) > 0:
        result = shard_levels(stream_key, extent, split, -0.22, 0.18) * result
    return jnp.clip(result, min=-most, max=most).astype(dtype)


def heavy_noise(stream_key, extent, spread, reach, pieces, heavy, kind=jnp.bfloat16):
    result = spread * jax.random.normal(stream_key, extent, jnp.float32)
    if pieces:
        result = result * shard_levels(stream_key, extent, pieces, -0.22, 0.18)
    return jnp.clip(spiked(result, jax.random.fold_in(stream_key, 3), *heavy), -reach, reach).astype(kind)


def setup_inputs(seed: int = 0) -> dict:
    splits = jax.random.split(jax.random.key(seed), 5)
    train_gate = heavy_noise(splits[0], (EXPERTS, D_MODEL, D_EXPERT), D_MODEL ** -0.5, 0.1875, ((0, 4), (1, 8)), (1, 2, 8, 2.0), jnp.float32)
    train_up = heavy_noise(splits[1], (EXPERTS, D_MODEL, D_EXPERT), D_MODEL ** -0.5, 0.1875, ((0, 4), (1, 8)), (1, 2, 8, 2.0), jnp.float32)
    router_weight = noise(splits[2], (D_MODEL, EXPERTS), D_MODEL ** -0.5, 0.125, ((0, 8), (1, 4)), jnp.float32)
    router_gain = jnp.clip(1.0 + 0.15 * jax.random.normal(splits[3], (D_MODEL,), jnp.float32), 0.25, 1.75)
    return dict(train_gate=train_gate, train_up=train_up, router_weight=router_weight, router_gain=router_gain)


def reference(train_gate, train_up, router_weight, router_gain):
    scale_gate = jnp.sqrt(lax.optimization_barrier(jnp.sum(train_gate * train_gate, axis=1)))
    ready_gate = (train_gate / jnp.expand_dims(scale_gate, 1)).astype(jnp.bfloat16)
    scale_up = jnp.sqrt(lax.optimization_barrier(jnp.sum(train_up * train_up, axis=1)))
    ready_up = (train_up / jnp.expand_dims(scale_up, 1)).astype(jnp.bfloat16)
    serve_router = (router_weight * router_gain[:, None]).astype(jnp.bfloat16)
    return (ready_gate, ready_up, scale_gate, scale_up, serve_router)
```

```python
import functools

import jax
import jax.numpy as jnp
from jax import lax
from jax.experimental import pallas as pl
from jax.experimental.pallas import tpu as pltpu
from jax.sharding import PartitionSpec as P

MESH = pl.DeviceIdType.MESH
CHUNK = 32


def split(n):
    return max(d for d in range(1, n + 1) if d * d <= n and n % d == 0)


def along(n, at, i):
    short = jnp.minimum(at, n - 1 - at)
    way = jnp.where(at < n - 1 - at, 1, -1)
    near = (i + 1) // 2 if i % 2 else -(i // 2)
    step = jnp.where(i <= 2 * short, near, i - short) * way
    return at + step, jnp.abs(step)


def routes(n, me):
    wide = split(n)
    deep = n // wide
    z, y = me // wide, lax.rem(me, wide)
    place, reach = [me], [0]
    for i in range(1, deep):
        other, far = along(deep, z, i)
        for j in range(wide):
            place.append(other * wide + lax.rem(y + j, wide))
            reach.append((far, (i + 1) // 2, i))
    for j in range(1, wide):
        place.append(z * wide + lax.rem(y + j, wide))
        reach.append(0)
    return deep, place, reach


def kernel(
    rows_n, owners_n,
    gate, up, weight, gain,
    ready_gate, ready_up, scale, router,
    slabs, send, part, gathered, scales, mine,
    load_sem, data_send, data_recv, sum_send, sum_recv, scale_send, scale_recv,
    own_sem, router_send, router_recv, router_own, forward_send, forward_recv,
):
    me, group = lax.axis_index("rows"), lax.axis_index("owner")
    height, width = gate.shape[2], gate.shape[3]
    each = gate.shape[1]
    steps = 2 * each
    deep, place, reach = routes(rows_n, me)
    peers = list(range(1, rows_n))
    order = peers + [0]
    here = pl.ds(pl.multiple_of(me * height, height), height)

    def load(step, slab):
        bank, c = (gate, up)[step // each], step % each
        return [
            pltpu.make_async_copy(bank.at[place[k], c], slabs.at[slab, k], load_sem.at[slab, k])
            for k in range(rows_n)
        ]

    def begin(copies):
        for copy in copies:
            copy.start()

    def sum_one(slab, k, step):
        def add(i, total):
            x = slabs[slab, k, pl.ds(i * CHUNK, CHUNK), :]
            return total + jnp.sum((x * x).reshape(CHUNK // 8, 8, width), axis=0)

        total = lax.fori_loop(0, height // CHUNK, add, jnp.zeros((8, width), jnp.float32))
        part[place[k], step] = jnp.sum(total, axis=0, keepdims=True)

    def sum_copies(which, lo, hi, arriving=False):
        return [
            pltpu.make_async_remote_copy(
                part.at[place[k], pl.ds(lo, hi - lo)],
                gathered.at[me, pl.ds(lo, hi - lo)],
                sum_send.at[which, k], sum_recv.at[which, place[k] if arriving else me],
                device_id={"rows": place[k]}, device_id_type=MESH,
            )
            for k in peers
        ]

    def scale_copies(which, lo, hi, arriving=False):
        return [
            pltpu.make_async_remote_copy(
                scales.at[me, pl.ds(lo, hi - lo)],
                scales.at[me, pl.ds(lo, hi - lo)],
                scale_send.at[which, k], scale_recv.at[which, place[k] if arriving else me],
                device_id={"rows": place[k]}, device_id_type=MESH,
            )
            for k in peers
        ]

    def arrive(copies):
        for copy in copies:
            copy.wait_recv()

    def finish_sums(lo, hi):
        for step in range(lo, hi):
            gathered[me, step] = part[me, step]
        for step in range(lo, hi):
            total = gathered[0, step]
            for source in range(1, rows_n):
                total = total + gathered[source, step]
            root = jnp.sqrt(total)
            scales[me, step] = root
            scale[step] = root

    def data_copy(step, k, arriving=False):
        bank, c = (ready_gate, ready_up)[step // each], step % each
        if k == 0:
            return pltpu.make_async_copy(send.at[step, 0], bank.at[c, here], own_sem.at[step])
        return pltpu.make_async_remote_copy(
            send.at[step, k], bank.at[c, here],
            data_send.at[step, k], data_recv.at[step, place[k] if arriving else me],
            device_id={"rows": place[k]}, device_id_type=MESH,
        )

    def narrow(slab, k, step):
        by = scales[place[k], step]

        def one(i, carry):
            at = pl.ds(i * CHUNK, CHUNK)
            send[step, k, at, :] = (slabs[slab, k, at, :] / by).astype(jnp.bfloat16)
            return carry

        lax.fori_loop(0, height // CHUNK, one, 0)

    def ship(slab, k, step):
        narrow(slab, k, step)
        data_copy(step, k).start()

    def start_at(distance, step):
        for k in peers:
            if reach[k] == 0:
                continue
            far, least, most = reach[k]
            if least <= distance <= most:
                @pl.when(far == distance)
                def _():
                    data_copy(step, k).start()

    first, second = load(0, 0), load(1, 1)
    begin(first)
    begin(second)

    barrier = pltpu.get_barrier_semaphore()
    for k in range(1, rows_n):
        pl.semaphore_signal(barrier, inc=1, device_id={"rows": place[k]}, device_id_type=MESH)
    for j in range(1, owners_n):
        pl.semaphore_signal(
            barrier, inc=1, device_id={"owner": lax.rem(group + j, owners_n)}, device_id_type=MESH
        )

    mine[...] = (weight[...] * gain[...]).astype(jnp.bfloat16)

    for k in order:
        first[k].wait()
        sum_one(0, k, 0)
    pl.semaphore_wait(barrier, rows_n + owners_n - 2)
    first_sums = sum_copies(0, 0, 1)
    begin(first_sums)
    arrive(sum_copies(0, 0, 1, True))
    finish_sums(0, 1)
    first_scales = scale_copies(0, 0, 1)
    begin(first_scales)
    arrive(scale_copies(0, 0, 1, True))

    half, rest = rows_n // 2, rows_n // 2 + rows_n // 8
    lots = order[:half], order[half:rest], order[rest:]
    for k in lots[0]:
        ship(0, k, 0)

    columns = pl.ds(pl.multiple_of(me * height, height), height)
    def router_copies(arriving=False):
        return [
            pltpu.make_async_remote_copy(
                mine, router.at[group, :, columns],
                router_send.at[k], router_recv.at[place[k] if arriving else me],
                device_id={"rows": place[k]}, device_id_type=MESH,
            )
            for k in peers
        ]

    router_local = pltpu.make_async_copy(mine, router.at[group, :, columns], router_own)
    router_local.start()

    waiting = second
    for step in range(1, steps):
        slab = 1 + (step - 1) % 2
        now = waiting
        if step + 1 < steps:
            waiting = load(step + 1, 1 + step % 2)
            begin(waiting)
        for k in range(rows_n):
            now[k].wait()
            sum_one(slab, k, step)
    rest_sums = sum_copies(1, 1, steps)
    begin(rest_sums)
    router_out = router_copies()
    begin(router_out)
    waiting = load(1, 1)
    begin(waiting)
    for k in lots[1]:
        ship(0, k, 0)
    arrive(sum_copies(1, 1, steps, True))
    finish_sums(1, steps)
    rest_scales = scale_copies(1, 1, steps)
    begin(rest_scales)
    for k in lots[2]:
        ship(0, k, 0)
    arrive(scale_copies(1, 1, steps, True))

    for step in range(1, steps):
        slab = 1 + (step - 1) % 2
        now = waiting
        if step + 1 < steps:
            waiting = load(step + 1, 1 + step % 2)
            begin(waiting)
        for k in order:
            now[k].wait()
            narrow(slab, k, step)
        start_at(1, step)
        data_copy(step, 0).start()
    for distance in range(2, deep):
        for step in range(1, steps):
            start_at(distance, step)
            if distance == 2:
                for k in peers:
                    if reach[k] == 0:
                        data_copy(step, k).start()

    arrive(router_copies(True))
    router_local.wait()
    forwards = []
    for j in range(1, owners_n):
        forwards.append(
            pltpu.make_async_remote_copy(
                router.at[group], router.at[group], forward_send.at[j], forward_recv.at[j],
                device_id={"owner": lax.rem(group + j, owners_n)}, device_id_type=MESH,
            )
        )
    begin(forwards)

    for copies in (first_sums, first_scales, rest_sums, rest_scales, router_out):
        for copy in copies:
            copy.wait_send()
    for copy in forwards:
        copy.wait()
    for step in range(steps):
        data_copy(step, 0).wait()
        for k in peers:
            data_copy(step, k).wait_send()
            data_copy(step, k, True).wait_recv()


def on_device(rows_n, owners_n, train_gate, train_up, router_weight, router_gain):
    experts, height, width = train_gate.shape
    each = experts // rows_n
    steps = 2 * each
    cols = router_weight.shape[1]
    f32, bf16, dma = jnp.float32, jnp.bfloat16, pltpu.SemaphoreType.DMA
    hbm, vmem = pl.BlockSpec(memory_space=pl.ANY), pl.BlockSpec(memory_space=pltpu.VMEM)
    ready = jax.ShapeDtypeStruct((each, rows_n * height, width), bf16)
    ready_gate, ready_up, scale, router = pl.pallas_call(
        functools.partial(kernel, rows_n, owners_n),
        out_shape=(
            ready,
            ready,
            jax.ShapeDtypeStruct((steps, 1, width), f32),
            jax.ShapeDtypeStruct((owners_n, cols, rows_n * height), bf16),
        ),
        in_specs=[hbm, hbm, vmem, vmem],
        out_specs=(hbm, hbm, vmem, hbm),
        scratch_shapes=[
            pltpu.VMEM((3, rows_n, height, width), f32),
            pltpu.VMEM((steps, rows_n, height, width), bf16),
            pltpu.VMEM((rows_n, steps, 1, width), f32),
            pltpu.VMEM((rows_n, steps, 1, width), f32),
            pltpu.VMEM((rows_n, steps, 1, width), f32),
            pltpu.VMEM((cols, height), bf16),
            dma((3, rows_n)),
            dma((steps, rows_n)),
            dma((steps, rows_n)),
            dma((2, rows_n)),
            dma((2, rows_n)),
            dma((2, rows_n)),
            dma((2, rows_n)),
            dma((steps,)),
            dma((rows_n,)),
            dma((rows_n,)),
            dma,
            dma((owners_n,)),
            dma((owners_n,)),
        ],
        compiler_params=pltpu.CompilerParams(
            collective_id=0, has_side_effects=True, vmem_limit_bytes=60 * 1024 * 1024
        ),
        name="serve",
    )(
        train_gate.reshape(rows_n, each, height, width),
        train_up.reshape(rows_n, each, height, width),
        router_weight.T,
        router_gain[None, :],
    )
    serve_router = router.reshape(owners_n * cols, rows_n * height).T
    scale = scale.reshape(steps, width)
    return (ready_gate, ready_up, scale[:each], scale[each:], serve_router)


def solution(mesh):
    return jax.shard_map(
        functools.partial(on_device, mesh.shape["rows"], mesh.shape["owner"]),
        mesh=mesh,
        in_specs=(
            P("owner", "rows", None),
            P("owner", "rows", None),
            P("rows", "owner"),
            P("rows"),
        ),
        out_specs=(
            P(("owner", "rows"), None, None),
            P(("owner", "rows"), None, None),
            P(("owner", "rows"), None),
            P(("owner", "rows"), None),
            P(),
        ),
        check_vma=False,
    )
```

```python
import functools

import jax
import jax.numpy as jnp
from jax import lax
from jax.experimental import pallas as pl
from jax.experimental.pallas import tpu as pltpu
from jax.sharding import PartitionSpec as P

MESH = pl.DeviceIdType.MESH
CHUNK = 32
RING = 10


def split(n):
    return max(d for d in range(1, n + 1) if d * d <= n and n % d == 0)


def across_first(n):
    if n == 1:
        return []
    half = n // 2
    return list(range(half, n)) + across_first(half)


def partner(n, at, k):
    if n & (n - 1):
        return lax.rem(at + k, n)
    other, bit = 0, 1
    while bit < n:
        own = (at // bit) % 2
        other = other + bit * ((1 - own) if k & bit else own)
        bit *= 2
    return other


def routes(n, me):
    wide = split(n)
    deep = n // wide
    z, y = me // wide, lax.rem(me, wide)
    place, groups = [me], []
    for far in across_first(deep) + [0]:
        group = []
        for near in range(wide):
            if far or near:
                group.append(len(place))
                place.append(partner(deep, z, far) * wide + partner(wide, y, near))
        groups.append(group)
    return place, groups


def kernel(
    rows_n, owners_n,
    gate, up, weight, gain,
    ready, scale, router,
    slabs, send, part, gathered, scales, mine,
    load_sem, data_send, data_recv, sum_send, sum_recv, scale_send, scale_recv,
    router_send, router_recv, forward_send, forward_recv,
):
    me, group = lax.axis_index("rows"), lax.axis_index("owner")
    height, width = gate.shape[2], gate.shape[3]
    each = gate.shape[1]
    steps = 2 * each
    place, groups = routes(rows_n, me)
    peers = list(range(1, rows_n))
    order = peers + [0]
    here = pl.ds(pl.multiple_of(me * height, height), height)

    pieces = [(step, k) for step in range(1, steps) for k in order]
    turns = pieces + pieces

    def load(slot, step, k):
        bank, c = (gate, up)[step // each], step % each
        return pltpu.make_async_copy(bank.at[place[k], c], slabs.at[slot], load_sem.at[slot])

    def turn_copy(t):
        return load(rows_n + t % RING, *turns[t])

    def begin(copies):
        for copy in copies:
            copy.start()

    def sum_one(slot, k, step):
        def add(i, total):
            x = slabs[slot, pl.ds(i * CHUNK, CHUNK), :]
            return total + jnp.sum((x * x).reshape(CHUNK // 8, 8, width), axis=0)

        total = lax.fori_loop(0, height // CHUNK, add, jnp.zeros((8, width), jnp.float32))
        part[place[k], step] = jnp.sum(total, axis=0, keepdims=True)

    def sum_copies(which, lo, hi, arriving=False):
        return [
            pltpu.make_async_remote_copy(
                part.at[place[k], pl.ds(lo, hi - lo)],
                gathered.at[me, pl.ds(lo, hi - lo)],
                sum_send.at[which, k], sum_recv.at[which, place[k] if arriving else me],
                device_id={"rows": place[k]}, device_id_type=MESH,
            )
            for k in peers
        ]

    def scale_copies(which, lo, hi, arriving=False):
        return [
            pltpu.make_async_remote_copy(
                scales.at[me, pl.ds(lo, hi - lo)],
                scales.at[me, pl.ds(lo, hi - lo)],
                scale_send.at[which, k], scale_recv.at[which, place[k] if arriving else me],
                device_id={"rows": place[k]}, device_id_type=MESH,
            )
            for k in peers
        ]

    def arrive(copies):
        for copy in copies:
            copy.wait_recv()

    def finish_sums(lo, hi):
        for step in range(lo, hi):
            gathered[me, step] = part[me, step]
        for step in range(lo, hi):
            total = gathered[0, step]
            for source in range(1, rows_n):
                total = total + gathered[source, step]
            root = jnp.sqrt(total)
            scales[me, step] = root
            scale[step] = root

    def data_copy(step, k, arriving=False):
        return pltpu.make_async_remote_copy(
            send.at[step, k - 1], ready.at[step, here],
            data_send.at[step, k], data_recv.at[step, place[k] if arriving else me],
            device_id={"rows": place[k]}, device_id_type=MESH,
        )

    def narrow(slot, k, step):
        by = scales[place[k], step]

        def one(i, carry):
            at = pl.ds(i * CHUNK, CHUNK)
            ready_rows = pl.ds(pl.multiple_of(me * height + i * CHUNK, CHUNK), CHUNK)
            value = (slabs[slot, at, :] / by).astype(jnp.bfloat16)
            if k == 0:
                ready[step, ready_rows, :] = value
            else:
                send[step, k - 1, at, :] = value
            return carry

        lax.fori_loop(0, height // CHUNK, one, 0)

    def send_group(lot, step):
        for k in lot:
            data_copy(step, k).start()

    for k in order:
        load(k, 0, k).start()
    for t in range(RING):
        turn_copy(t).start()

    barrier = pltpu.get_barrier_semaphore()
    for k in range(1, rows_n):
        pl.semaphore_signal(barrier, inc=1, device_id={"rows": place[k]}, device_id_type=MESH)
    for j in range(1, owners_n):
        pl.semaphore_signal(
            barrier, inc=1, device_id={"owner": lax.rem(group + j, owners_n)}, device_id_type=MESH
        )

    mine[...] = (weight[...] * gain[...]).astype(jnp.bfloat16)

    for k in order:
        load(k, 0, k).wait()
        sum_one(k, k, 0)
    pl.semaphore_wait(barrier, rows_n + owners_n - 2)
    first_sums = sum_copies(0, 0, 1)
    begin(first_sums)
    arrive(sum_copies(0, 0, 1, True))
    finish_sums(0, 1)
    first_scales = scale_copies(0, 0, 1)
    begin(first_scales)
    arrive(scale_copies(0, 0, 1, True))

    lots = groups[0], groups[1][:1], groups[1][1:]
    later = [k for lot in groups[2:] for k in lot] + [0]
    for k in lots[0]:
        narrow(k, k, 0)
        data_copy(0, k).start()

    columns = pl.ds(pl.multiple_of(me * height, height), height)

    def router_copies(arriving=False):
        return [
            pltpu.make_async_remote_copy(
                mine, router.at[group, :, columns],
                router_send.at[k], router_recv.at[place[k] if arriving else me],
                device_id={"rows": place[k]}, device_id_type=MESH,
            )
            for k in peers
        ]

    router[group, :, columns] = mine[...]

    def take(t, use):
        step, k = turns[t]
        turn_copy(t).wait()
        use(rows_n + t % RING, k, step)
        if t + RING < len(turns):
            turn_copy(t + RING).start()

    for t in range(len(pieces)):
        take(t, sum_one)
    rest_sums = sum_copies(1, 1, steps)
    begin(rest_sums)
    router_out = router_copies()
    begin(router_out)
    for k in lots[1]:
        narrow(k, k, 0)
        data_copy(0, k).start()
    arrive(sum_copies(1, 1, steps, True))
    finish_sums(1, steps)
    rest_scales = scale_copies(1, 1, steps)
    begin(rest_scales)
    for k in lots[2]:
        narrow(k, k, 0)
        data_copy(0, k).start()
    for k in later:
        narrow(k, k, 0)
    arrive(scale_copies(1, 1, steps, True))

    for step in range(1, steps):
        for i in range(rows_n):
            take(len(pieces) + (step - 1) * rows_n + i, narrow)
        send_group(groups[0], step)
    for i, lot in enumerate(groups[1:]):
        for step in range(0 if i else 1, steps):
            send_group(lot, step)

    arrive(router_copies(True))
    forwards = []
    for j in range(1, owners_n):
        forwards.append(
            pltpu.make_async_remote_copy(
                router.at[group], router.at[group], forward_send.at[j], forward_recv.at[j],
                device_id={"owner": lax.rem(group + j, owners_n)}, device_id_type=MESH,
            )
        )
    begin(forwards)

    for copies in (first_sums, first_scales, rest_sums, rest_scales, router_out):
        for copy in copies:
            copy.wait_send()
    for copy in forwards:
        copy.wait()
    for step in range(steps):
        for k in peers:
            data_copy(step, k).wait_send()
            data_copy(step, k, True).wait_recv()


def finish(each, ready, scale, router, ready_gate, ready_up, scale_gate, scale_up, serve_router, sem):
    banks = ready_gate, ready_up
    copies = [
        pltpu.make_async_copy(ready.at[step], banks[step // each].at[step % each], sem.at[step])
        for step in range(2 * each)
    ]
    for copy in copies:
        copy.start()
    scale_gate[...] = scale[pl.ds(0, each)].reshape(scale_gate.shape)
    scale_up[...] = scale[pl.ds(each, each)].reshape(scale_up.shape)
    owners, cols, rows = router.shape
    serve_router[...] = router[...].reshape(owners * cols, rows).T
    for copy in copies:
        copy.wait()


def on_device(rows_n, owners_n, train_gate, train_up, router_weight, router_gain):
    experts, height, width = train_gate.shape
    each = experts // rows_n
    steps = 2 * each
    cols = router_weight.shape[1]
    f32, bf16, dma = jnp.float32, jnp.bfloat16, pltpu.SemaphoreType.DMA
    hbm, vmem = pl.BlockSpec(memory_space=pl.ANY), pl.BlockSpec(memory_space=pltpu.VMEM)
    landing = 2 * steps * rows_n * height * width
    ready, scale, router = pl.pallas_call(
        functools.partial(kernel, rows_n, owners_n),
        out_shape=(
            pltpu.VMEM((steps, rows_n * height, width), bf16),
            pltpu.VMEM((steps, 1, width), f32),
            pltpu.VMEM((owners_n, cols, rows_n * height), bf16),
        ),
        in_specs=[hbm, hbm, vmem, vmem],
        out_specs=(vmem, vmem, vmem),
        scratch_shapes=[
            pltpu.VMEM((rows_n + RING, height, width), f32),
            pltpu.VMEM((steps, rows_n - 1, height, width), bf16),
            pltpu.VMEM((rows_n, steps, 1, width), f32),
            pltpu.VMEM((rows_n, steps, 1, width), f32),
            pltpu.VMEM((rows_n, steps, 1, width), f32),
            pltpu.VMEM((cols, height), bf16),
            dma((rows_n + RING,)),
            dma((steps, rows_n)),
            dma((steps, rows_n)),
            dma((2, rows_n)),
            dma((2, rows_n)),
            dma((2, rows_n)),
            dma((2, rows_n)),
            dma((rows_n,)),
            dma((rows_n,)),
            dma((owners_n,)),
            dma((owners_n,)),
        ],
        compiler_params=pltpu.CompilerParams(
            collective_id=0, has_side_effects=True, vmem_limit_bytes=61 * 1024 * 1024 - landing
        ),
        name="serve",
    )(
        train_gate.reshape(rows_n, each, height, width),
        train_up.reshape(rows_n, each, height, width),
        router_weight.T,
        router_gain[None, :],
    )
    bank = jax.ShapeDtypeStruct((each, rows_n * height, width), bf16)
    scales = jax.ShapeDtypeStruct((each, width), f32)
    return pl.pallas_call(
        functools.partial(finish, each),
        out_shape=(bank, bank, scales, scales, jax.ShapeDtypeStruct((rows_n * height, owners_n * cols), bf16)),
        in_specs=[vmem, vmem, vmem],
        out_specs=(hbm, hbm, vmem, vmem, vmem),
        scratch_shapes=[dma((steps,))],
        compiler_params=pltpu.CompilerParams(vmem_limit_bytes=8 * 1024 * 1024),
        name="finish",
    )(ready, scale, router)


def solution(mesh):
    return jax.shard_map(
        functools.partial(on_device, mesh.shape["rows"], mesh.shape["owner"]),
        mesh=mesh,
        in_specs=(
            P("owner", "rows", None),
            P("owner", "rows", None),
            P("rows", "owner"),
            P("rows"),
        ),
        out_specs=(
            P(("owner", "rows"), None, None),
            P(("owner", "rows"), None, None),
            P(("owner", "rows"), None),
            P(("owner", "rows"), None),
            P(),
        ),
        check_vma=False,
    )
```

```python
import functools

import jax
import jax.numpy as jnp
from jax import lax
from jax.experimental import pallas as pl
from jax.experimental.pallas import tpu as pltpu
from jax.sharding import PartitionSpec as P

MESH = pl.DeviceIdType.MESH
CHUNK = 32
RING = 10


def split(n):
    return max(d for d in range(1, n + 1) if d * d <= n and n % d == 0)


def across_first(n):
    if n == 1:
        return []
    half = n // 2
    return list(range(half, n)) + across_first(half)


def partner(at, k):
    other, bit = at, 1
    while bit <= k:
        if k & bit:
            other = other + bit * (1 - 2 * ((at // bit) % 2))
        bit *= 2
    return other


def routes(n, me):
    wide = split(n)
    deep = n // wide
    z, y = me // wide, lax.rem(me, wide)
    place, groups = [me], []
    for far in across_first(deep) + [0]:
        group = []
        for near in range(wide):
            if far or near:
                group.append(len(place))
                place.append(partner(z, far) * wide + partner(y, near))
        groups.append(group)
    return wide, place, groups


def kernel(
    rows_n, owners_n,
    gate, up, weight, gain,
    ready, scale, router,
    slabs, send, part, gathered, relayed, halves, other, first, first_by, scales, mine,
    load_sem, data_send, data_recv, sum_send, sum_recv, first_send, first_recv, scale_send, scale_recv,
    relay_send, relay_recv, cross_send, cross_recv, spread_send, spread_recv,
    router_send, router_recv, forward_send, forward_recv,
):
    me, group = lax.axis_index("rows"), lax.axis_index("owner")
    height, width = gate.shape[2], gate.shape[3]
    each = gate.shape[1]
    steps = 2 * each
    wide, place, groups = routes(rows_n, me)
    half = rows_n // 2
    close = [k for lot in groups[half // wide :] for k in lot]
    mate, side = place[1], (me // half) * half
    peers = list(range(1, rows_n))
    order = peers + [0]
    here = pl.ds(pl.multiple_of(me * height, height), height)

    pieces = [(step, k) for step in range(1, steps) for k in order]
    turns = pieces + pieces

    def load(slot, step, k):
        bank, c = (gate, up)[step // each], step % each
        return pltpu.make_async_copy(bank.at[place[k], c], slabs.at[slot], load_sem.at[slot])

    def turn_copy(t):
        return load(rows_n + t % RING, *turns[t])

    def begin(copies):
        for copy in copies:
            copy.start()

    def sum_one(slot, k, step):
        def add(i, total):
            x = slabs[slot, pl.ds(i * CHUNK, CHUNK), :]
            return total + jnp.sum((x * x).reshape(CHUNK // 8, 8, width), axis=0)

        total = lax.fori_loop(0, height // CHUNK, add, jnp.zeros((8, width), jnp.float32))
        part[place[k], step] = jnp.sum(total, axis=0, keepdims=True)

    def to_peer(source, target, out_sem, in_sem, k):
        return pltpu.make_async_remote_copy(
            source, target, out_sem, in_sem, device_id={"rows": place[k]}, device_id_type=MESH
        )

    def sum_copies(arriving=False):
        return [
            to_peer(
                part.at[place[k], pl.ds(0, 1)], gathered.at[me, pl.ds(0, 1)],
                sum_send.at[k], sum_recv.at[place[k] if arriving else me], k,
            )
            for k in peers
        ]

    def ahead(device):
        return pl.ds(partner(device // wide, half // wide) * wide, wide)

    def first_copies(arriving=False):
        return [
            to_peer(
                part.at[ahead(place[k]), 0], first.at[me],
                first_send.at[k], first_recv.at[place[k] if arriving else me], k,
            )
            for k in peers
        ]

    def scale_copies(arriving=False):
        return [
            to_peer(
                scales.at[me, pl.ds(0, 1)], scales.at[me, pl.ds(0, 1)],
                scale_send.at[k], scale_recv.at[place[k] if arriving else me], k,
            )
            for k in peers
        ]

    rest = pl.ds(1, steps - 1)

    def relay_copies(arriving=False):
        return [
            to_peer(
                part.at[device, rest], bank.at[me, rest],
                relay_send.at[which, k], relay_recv.at[which, place[k] if arriving else me], k,
            )
            for k in close
            for which, (bank, device) in enumerate(
                ((gathered, place[k]), (relayed, partner(place[k] // wide, half // wide) * wide + lax.rem(place[k], wide)))
            )
        ]

    def spread_copies(arriving=False):
        return [
            to_peer(
                scales.at[device, rest], scales.at[device, rest],
                spread_send.at[which, k], spread_recv.at[which, place[k] if arriving else me], k,
            )
            for k in close
            for which, device in enumerate((me, mate))
        ]

    def arrive(copies):
        for copy in copies:
            copy.wait_recv()

    def finish_first():
        gathered[me, 0] = part[me, 0]
        first[me] = part[ahead(me), 0]
        total, forward = gathered[0, 0], first[0]
        for source in range(1, rows_n):
            total = total + gathered[source, 0]
            forward = forward + first[source]
        root = jnp.sqrt(total)
        scales[me, 0] = root
        scale[0] = root
        first_by[...] = jnp.sqrt(forward)

    def halve():
        gathered[me, rest] = part[me, rest]
        relayed[me, rest] = part[mate, rest]
        for which, bank in enumerate((gathered, relayed)):
            total = bank[side, rest]
            for i in range(1, half):
                total = total + bank[side + i, rest]
            halves[which] = total

    def finish_rest():
        root = jnp.sqrt(halves[0] + other[1])
        scales[me, rest] = root
        scale[rest] = root
        scales[mate, rest] = jnp.sqrt(halves[1] + other[0])

    def data_copy(step, k, arriving=False):
        return pltpu.make_async_remote_copy(
            send.at[step, k - 1], ready.at[step, here],
            data_send.at[step, k], data_recv.at[step, place[k] if arriving else me],
            device_id={"rows": place[k]}, device_id_type=MESH,
        )

    def narrow(slot, k, step, by=None):
        by = scales[place[k], step] if by is None else by

        def one(i, carry):
            at = pl.ds(i * CHUNK, CHUNK)
            ready_rows = pl.ds(pl.multiple_of(me * height + i * CHUNK, CHUNK), CHUNK)
            value = (slabs[slot, at, :] / by).astype(jnp.bfloat16)
            if k == 0:
                ready[step, ready_rows, :] = value
            else:
                send[step, k - 1, at, :] = value
            return carry

        lax.fori_loop(0, height // CHUNK, one, 0)

    def send_group(lot, step):
        for k in lot:
            data_copy(step, k).start()

    for k in order:
        load(k, 0, k).start()

    barrier = pltpu.get_barrier_semaphore()
    for k in peers:
        pl.semaphore_signal(barrier, inc=1, device_id={"rows": place[k]}, device_id_type=MESH)
    for j in range(1, owners_n):
        pl.semaphore_signal(
            barrier, inc=1, device_id={"owner": lax.rem(group + j, owners_n)}, device_id_type=MESH
        )

    columns = pl.ds(pl.multiple_of(me * height, height), height)
    mine[...] = (weight[...] * gain[...]).astype(jnp.bfloat16)
    router[group, :, columns] = mine[...]

    def router_copies(arriving=False):
        return [
            to_peer(
                mine, router.at[group, :, columns],
                router_send.at[k], router_recv.at[place[k] if arriving else me], k,
            )
            for k in peers
        ]

    pl.semaphore_wait(barrier, rows_n + owners_n - 2)
    router_out = router_copies()
    begin(router_out)

    for k in order:
        load(k, 0, k).wait()
        sum_one(k, k, 0)
    sums_out, first_out = sum_copies(), first_copies()
    begin(first_out)
    begin(sums_out)
    for t in range(RING):
        turn_copy(t).start()
    arrive(first_copies(True))
    arrive(sum_copies(True))
    finish_first()
    scales_out = scale_copies()
    begin(scales_out)

    def cover(k, by=None):
        narrow(k, k, 0, by)
        data_copy(0, k).start()

    covers = groups[0] + groups[1]
    cover(covers[0], first_by[lax.rem(place[covers[0]], wide)])

    def take(t, use):
        step, k = turns[t]
        turn_copy(t).wait()
        use(rows_n + t % RING, k, step)
        if t + RING < len(turns):
            turn_copy(t + RING).start()

    for t in range(len(pieces)):
        take(t, sum_one)
    relay_out = relay_copies()
    begin(relay_out)
    cover(covers[1], first_by[lax.rem(place[covers[1]], wide)])
    arrive(scale_copies(True))
    arrive(relay_copies(True))
    halve()
    cross = to_peer(halves, other, cross_send, cross_recv, 1)
    cross.start()
    cover(covers[2])
    cross.wait_recv()
    finish_rest()
    spread_out = spread_copies()
    begin(spread_out)
    for k in covers[3:]:
        cover(k)
    for k in order:
        if k not in covers:
            narrow(k, k, 0)
    arrive(spread_copies(True))

    for step in range(1, steps):
        for i in range(rows_n):
            take(len(pieces) + (step - 1) * rows_n + i, narrow)
        send_group(groups[0], step)
    for i, lot in enumerate(groups[1:]):
        for step in range(0 if i else 1, steps):
            send_group(lot, step)

    arrive(router_copies(True))
    forwards = []
    for j in range(1, owners_n):
        forwards.append(
            pltpu.make_async_remote_copy(
                router.at[group], router.at[group], forward_send.at[j], forward_recv.at[j],
                device_id={"owner": lax.rem(group + j, owners_n)}, device_id_type=MESH,
            )
        )
    begin(forwards)

    cross.wait_send()
    for copies in (first_out, sums_out, scales_out, relay_out, spread_out, router_out):
        for copy in copies:
            copy.wait_send()
    for copy in forwards:
        copy.wait()
    for step in range(steps):
        for k in peers:
            data_copy(step, k).wait_send()
            data_copy(step, k, True).wait_recv()


def finish(
    each, ready, scale, router,
    ready_gate, ready_up, scale_gate, scale_up, serve_router,
    low, high, turned, sem, small_sem,
):
    banks = ready_gate, ready_up
    copies = [
        pltpu.make_async_copy(ready.at[step], banks[step // each].at[step % each], sem.at[step])
        for step in range(2 * each)
    ]
    for copy in copies:
        copy.start()
    low[...] = scale[pl.ds(0, each)].reshape(low.shape)
    high[...] = scale[pl.ds(each, each)].reshape(high.shape)
    owners, cols, rows = router.shape
    turned[...] = router[...].reshape(owners * cols, rows).T
    small = [
        pltpu.make_async_copy(source, target, small_sem.at[i])
        for i, (source, target) in enumerate(
            ((low, scale_gate), (high, scale_up), (turned, serve_router))
        )
    ]
    for copy in small:
        copy.start()
    for copy in copies + small:
        copy.wait()


def on_device(rows_n, owners_n, train_gate, train_up, router_weight, router_gain):
    experts, height, width = train_gate.shape
    each = experts // rows_n
    steps = 2 * each
    cols = router_weight.shape[1]
    f32, bf16, dma = jnp.float32, jnp.bfloat16, pltpu.SemaphoreType.DMA
    hbm, vmem = pl.BlockSpec(memory_space=pl.ANY), pl.BlockSpec(memory_space=pltpu.VMEM)
    landing = 2 * steps * rows_n * height * width
    ready, scale, router = pl.pallas_call(
        functools.partial(kernel, rows_n, owners_n),
        out_shape=(
            pltpu.VMEM((steps, rows_n * height, width), bf16),
            pltpu.VMEM((steps, 1, width), f32),
            pltpu.VMEM((owners_n, cols, rows_n * height), bf16),
        ),
        in_specs=[hbm, hbm, vmem, vmem],
        out_specs=(vmem, vmem, vmem),
        scratch_shapes=[
            pltpu.VMEM((rows_n + RING, height, width), f32),
            pltpu.VMEM((steps, rows_n - 1, height, width), bf16),
            pltpu.VMEM((rows_n, steps, 1, width), f32),
            pltpu.VMEM((rows_n, steps, 1, width), f32),
            pltpu.VMEM((rows_n, steps, 1, width), f32),
            pltpu.VMEM((2, steps - 1, 1, width), f32),
            pltpu.VMEM((2, steps - 1, 1, width), f32),
            pltpu.VMEM((rows_n, split(rows_n), 1, width), f32),
            pltpu.VMEM((split(rows_n), 1, width), f32),
            pltpu.VMEM((rows_n, steps, 1, width), f32),
            pltpu.VMEM((cols, height), bf16),
            dma((rows_n + RING,)),
            dma((steps, rows_n)),
            dma((steps, rows_n)),
            dma((rows_n,)),
            dma((rows_n,)),
            dma((rows_n,)),
            dma((rows_n,)),
            dma((rows_n,)),
            dma((rows_n,)),
            dma((2, rows_n)),
            dma((2, rows_n)),
            dma,
            dma,
            dma((2, rows_n)),
            dma((2, rows_n)),
            dma((rows_n,)),
            dma((rows_n,)),
            dma((owners_n,)),
            dma((owners_n,)),
        ],
        compiler_params=pltpu.CompilerParams(
            collective_id=0, has_side_effects=True, vmem_limit_bytes=61 * 1024 * 1024 - landing
        ),
        name="serve",
    )(
        train_gate.reshape(rows_n, each, height, width),
        train_up.reshape(rows_n, each, height, width),
        router_weight.T,
        router_gain[None, :],
    )
    bank = jax.ShapeDtypeStruct((each, rows_n * height, width), bf16)
    scales = jax.ShapeDtypeStruct((each, width), f32)
    return pl.pallas_call(
        functools.partial(finish, each),
        out_shape=(bank, bank, scales, scales, jax.ShapeDtypeStruct((rows_n * height, owners_n * cols), bf16)),
        in_specs=[vmem, vmem, vmem],
        out_specs=(hbm, hbm, hbm, hbm, hbm),
        scratch_shapes=[
            pltpu.VMEM((each, width), f32),
            pltpu.VMEM((each, width), f32),
            pltpu.VMEM((rows_n * height, owners_n * cols), bf16),
            dma((steps,)),
            dma((3,)),
        ],
        compiler_params=pltpu.CompilerParams(vmem_limit_bytes=8 * 1024 * 1024),
        name="finish",
    )(ready, scale, router)


def solution(mesh):
    return jax.shard_map(
        functools.partial(on_device, mesh.shape["rows"], mesh.shape["owner"]),
        mesh=mesh,
        in_specs=(
            P("owner", "rows", None),
            P("owner", "rows", None),
            P("rows", "owner"),
            P("rows"),
        ),
        out_specs=(
            P(("owner", "rows"), None, None),
            P(("owner", "rows"), None, None),
            P(("owner", "rows"), None),
            P(("owner", "rows"), None),
            P(),
        ),
        check_vma=False,
    )
```

```python
import functools

import jax
import jax.numpy as jnp
from jax import lax
from jax.experimental import pallas as pl
from jax.experimental.pallas import tpu as pltpu
from jax.sharding import PartitionSpec as P

MESH = pl.DeviceIdType.MESH
CHUNK = 32
RING = 10
PARTS = 4


def split(n):
    return max(d for d in range(1, n + 1) if d * d <= n and n % d == 0)


def across_first(n):
    if n == 1:
        return []
    half = n // 2
    return list(range(half, n)) + across_first(half)


def partner(at, k):
    other, bit = at, 1
    while bit <= k:
        if k & bit:
            other = other + bit * (1 - 2 * ((at // bit) % 2))
        bit *= 2
    return other


def routes(n, me):
    wide = split(n)
    deep = n // wide
    z, y = me // wide, lax.rem(me, wide)
    place, groups = [me], []
    for far in across_first(deep) + [0]:
        group = []
        for near in range(wide):
            if far or near:
                group.append(len(place))
                place.append(partner(z, far) * wide + partner(y, near))
        groups.append(group)
    return wide, place, groups


def kernel(
    rows_n, owners_n,
    gate, up, weight, gain,
    ready, scale, router,
    slabs, send, part, gathered, relayed, halves, other, first, first_by, scales, mine,
    load_sem, data_send, data_recv, first_send, first_recv,
    relay_send, relay_recv, cross_send, cross_recv, spread_send, spread_recv,
    router_send, router_recv, forward_send, forward_recv,
):
    me, group = lax.axis_index("rows"), lax.axis_index("owner")
    height, width = gate.shape[2], gate.shape[3]
    each = gate.shape[1]
    steps = 2 * each
    wide, place, groups = routes(rows_n, me)
    half = rows_n // 2
    close = [k for lot in groups[half // wide :] for k in lot]
    mate, side = place[1], (me // half) * half
    peers = list(range(1, rows_n))
    order = peers + [0]
    here = pl.ds(pl.multiple_of(me * height, height), height)

    pieces = [(step, k) for step in range(1, steps) for k in order]
    turns = pieces + pieces

    def load(slot, step, k):
        bank, c = (gate, up)[step // each], step % each
        return pltpu.make_async_copy(bank.at[place[k], c], slabs.at[slot], load_sem.at[slot])

    def turn_copy(t):
        return load(rows_n + t % RING, *turns[t])

    def begin(copies):
        for copy in copies:
            copy.start()

    def sum_one(slot, k, step):
        def add(i, total):
            x = slabs[slot, pl.ds(i * CHUNK, CHUNK), :]
            return total + jnp.sum((x * x).reshape(CHUNK // 8, 8, width), axis=0)

        total = lax.fori_loop(0, height // CHUNK, add, jnp.zeros((8, width), jnp.float32))
        part[place[k], step] = jnp.sum(total, axis=0, keepdims=True)

    def to_peer(source, target, out_sem, in_sem, k):
        return pltpu.make_async_remote_copy(
            source, target, out_sem, in_sem, device_id={"rows": place[k]}, device_id_type=MESH
        )

    def ahead(device):
        return pl.ds(partner(device // wide, half // wide) * wide, wide)

    def first_copies(arriving=False):
        return [
            to_peer(
                part.at[ahead(place[k]), 0], first.at[me],
                first_send.at[k], first_recv.at[place[k] if arriving else me], k,
            )
            for k in peers
        ]

    def relay_copies(arriving=False):
        return [
            to_peer(
                part.at[device], bank.at[me],
                relay_send.at[which, k], relay_recv.at[which, place[k] if arriving else me], k,
            )
            for k in close
            for which, (bank, device) in enumerate(
                ((gathered, place[k]), (relayed, partner(place[k] // wide, half // wide) * wide + lax.rem(place[k], wide)))
            )
        ]

    def spread_copies(arriving=False):
        return [
            to_peer(
                scales.at[device], scales.at[device],
                spread_send.at[which, k], spread_recv.at[which, place[k] if arriving else me], k,
            )
            for k in close
            for which, device in enumerate((me, mate))
        ]

    def arrive(copies):
        for copy in copies:
            copy.wait_recv()

    def finish_first():
        first[me] = part[ahead(me), 0]
        total = [first[0], first[half]]
        for i in range(1, half):
            total = [total[0] + first[i], total[1] + first[half + i]]
        first_by[...] = jnp.sqrt(total[0] + total[1])

    def halve():
        gathered[me] = part[me]
        relayed[me] = part[mate]
        for which, bank in enumerate((gathered, relayed)):
            total = bank[side]
            for i in range(1, half):
                total = total + bank[side + i]
            halves[which] = total

    def finish_rest():
        root = jnp.sqrt(halves[0] + other[1])
        scales[me] = root
        scale[...] = root
        scales[mate] = jnp.sqrt(halves[1] + other[0])

    def data_copy(step, k, arriving=False):
        return pltpu.make_async_remote_copy(
            send.at[step, k - 1], ready.at[step, here],
            data_send.at[step, k], data_recv.at[step, place[k] if arriving else me],
            device_id={"rows": place[k]}, device_id_type=MESH,
        )

    def narrow(slot, k, step):
        by = scales[place[k], step]

        def one(i, carry):
            at = pl.ds(i * CHUNK, CHUNK)
            ready_rows = pl.ds(pl.multiple_of(me * height + i * CHUNK, CHUNK), CHUNK)
            value = (slabs[slot, at, :] / by).astype(jnp.bfloat16)
            if k == 0:
                ready[step, ready_rows, :] = value
            else:
                send[step, k - 1, at, :] = value
            return carry

        lax.fori_loop(0, height // CHUNK, one, 0)
        if k in groups[0]:
            data_copy(step, k).start()

    tall = height // PARTS

    def cover(turn):
        k, piece = turn % wide + 1, turn // wide
        by = first_by[lax.rem(place[k], wide)]
        at = pl.ds(piece * tall, tall)
        send[0, k - 1, at, :] = (slabs[k, at, :] / by).astype(jnp.bfloat16)
        to_peer(
            send.at[0, k - 1, at],
            ready.at[0, pl.ds(pl.multiple_of(me * height + piece * tall, tall), tall)],
            data_send.at[0, k], data_recv.at[0, me], k,
        ).start()

    def send_group(lot, step):
        for k in lot:
            data_copy(step, k).start()

    for k in order:
        load(k, 0, k).start()

    barrier = pltpu.get_barrier_semaphore()
    for k in peers:
        pl.semaphore_signal(barrier, inc=1, device_id={"rows": place[k]}, device_id_type=MESH)
    for j in range(1, owners_n):
        pl.semaphore_signal(
            barrier, inc=1, device_id={"owner": lax.rem(group + j, owners_n)}, device_id_type=MESH
        )

    columns = pl.ds(pl.multiple_of(me * height, height), height)
    mine[...] = (weight[...] * gain[...]).astype(jnp.bfloat16)
    router[group, :, columns] = mine[...]

    def router_copies(arriving=False):
        return [
            to_peer(
                mine, router.at[group, :, columns],
                router_send.at[k], router_recv.at[place[k] if arriving else me], k,
            )
            for k in peers
        ]

    pl.semaphore_wait(barrier, rows_n + owners_n - 2)

    for k in order:
        load(k, 0, k).wait()
        sum_one(k, k, 0)
    first_out = first_copies()
    begin(first_out)
    router_out = router_copies()
    begin(router_out)
    for t in range(RING):
        turn_copy(t).start()
    arrive(first_copies(True))
    finish_first()
    covers = PARTS * wide
    for turn in range(covers // 2):
        cover(turn)

    def take(t, use):
        step, k = turns[t]
        turn_copy(t).wait()
        use(rows_n + t % RING, k, step)
        if t + RING < len(turns):
            turn_copy(t + RING).start()

    for t in range(len(pieces)):
        take(t, sum_one)
    relay_out = relay_copies()
    begin(relay_out)
    cover(covers // 2)
    arrive(relay_copies(True))
    halve()
    cross = to_peer(halves, other, cross_send, cross_recv, 1)
    cross.start()
    cover(covers // 2 + 1)
    cross.wait_recv()
    finish_rest()
    spread_out = spread_copies()
    begin(spread_out)
    for turn in range(covers // 2 + 2, covers):
        cover(turn)
    arrive(spread_copies(True))

    for t in range(len(pieces), len(turns)):
        take(t, narrow)
    for k in order:
        if k not in groups[0]:
            narrow(k, k, 0)
    for lot in groups[1:]:
        for step in range(steps):
            send_group(lot, step)

    arrive(router_copies(True))
    forwards = []
    for j in range(1, owners_n):
        forwards.append(
            pltpu.make_async_remote_copy(
                router.at[group], router.at[group], forward_send.at[j], forward_recv.at[j],
                device_id={"owner": lax.rem(group + j, owners_n)}, device_id_type=MESH,
            )
        )
    begin(forwards)

    cross.wait_send()
    for copies in (first_out, relay_out, spread_out, router_out):
        for copy in copies:
            copy.wait_send()
    for copy in forwards:
        copy.wait()
    for step in range(steps):
        for k in peers:
            data_copy(step, k).wait_send()
            data_copy(step, k, True).wait_recv()


def finish(
    each, ready, scale, router,
    ready_gate, ready_up, scale_gate, scale_up, serve_router,
    low, high, turned, sem, small_sem,
):
    banks = ready_gate, ready_up
    copies = [
        pltpu.make_async_copy(ready.at[step], banks[step // each].at[step % each], sem.at[step])
        for step in range(2 * each)
    ]
    for copy in copies:
        copy.start()
    low[...] = scale[pl.ds(0, each)].reshape(low.shape)
    high[...] = scale[pl.ds(each, each)].reshape(high.shape)
    owners, cols, rows = router.shape
    turned[...] = router[...].reshape(owners * cols, rows).T
    small = [
        pltpu.make_async_copy(source, target, small_sem.at[i])
        for i, (source, target) in enumerate(
            ((low, scale_gate), (high, scale_up), (turned, serve_router))
        )
    ]
    for copy in small:
        copy.start()
    for copy in copies + small:
        copy.wait()


def on_device(rows_n, owners_n, train_gate, train_up, router_weight, router_gain):
    experts, height, width = train_gate.shape
    each = experts // rows_n
    steps = 2 * each
    cols = router_weight.shape[1]
    f32, bf16, dma = jnp.float32, jnp.bfloat16, pltpu.SemaphoreType.DMA
    hbm, vmem = pl.BlockSpec(memory_space=pl.ANY), pl.BlockSpec(memory_space=pltpu.VMEM)
    landing = 2 * steps * rows_n * height * width
    ready, scale, router = pl.pallas_call(
        functools.partial(kernel, rows_n, owners_n),
        out_shape=(
            pltpu.VMEM((steps, rows_n * height, width), bf16),
            pltpu.VMEM((steps, 1, width), f32),
            pltpu.VMEM((owners_n, cols, rows_n * height), bf16),
        ),
        in_specs=[hbm, hbm, vmem, vmem],
        out_specs=(vmem, vmem, vmem),
        scratch_shapes=[
            pltpu.VMEM((rows_n + RING, height, width), f32),
            pltpu.VMEM((steps, rows_n - 1, height, width), bf16),
            pltpu.VMEM((rows_n, steps, 1, width), f32),
            pltpu.VMEM((rows_n, steps, 1, width), f32),
            pltpu.VMEM((rows_n, steps, 1, width), f32),
            pltpu.VMEM((2, steps, 1, width), f32),
            pltpu.VMEM((2, steps, 1, width), f32),
            pltpu.VMEM((rows_n, split(rows_n), 1, width), f32),
            pltpu.VMEM((split(rows_n), 1, width), f32),
            pltpu.VMEM((rows_n, steps, 1, width), f32),
            pltpu.VMEM((cols, height), bf16),
            dma((rows_n + RING,)),
            dma((steps, rows_n)),
            dma((steps, rows_n)),
            dma((rows_n,)),
            dma((rows_n,)),
            dma((2, rows_n)),
            dma((2, rows_n)),
            dma,
            dma,
            dma((2, rows_n)),
            dma((2, rows_n)),
            dma((rows_n,)),
            dma((rows_n,)),
            dma((owners_n,)),
            dma((owners_n,)),
        ],
        compiler_params=pltpu.CompilerParams(
            collective_id=0, has_side_effects=True, vmem_limit_bytes=61 * 1024 * 1024 - landing
        ),
        name="serve",
    )(
        train_gate.reshape(rows_n, each, height, width),
        train_up.reshape(rows_n, each, height, width),
        router_weight.T,
        router_gain[None, :],
    )
    bank = jax.ShapeDtypeStruct((each, rows_n * height, width), bf16)
    scales = jax.ShapeDtypeStruct((each, width), f32)
    return pl.pallas_call(
        functools.partial(finish, each),
        out_shape=(bank, bank, scales, scales, jax.ShapeDtypeStruct((rows_n * height, owners_n * cols), bf16)),
        in_specs=[vmem, vmem, vmem],
        out_specs=(hbm, hbm, hbm, hbm, hbm),
        scratch_shapes=[
            pltpu.VMEM((each, width), f32),
            pltpu.VMEM((each, width), f32),
            pltpu.VMEM((rows_n * height, owners_n * cols), bf16),
            dma((steps,)),
            dma((3,)),
        ],
        compiler_params=pltpu.CompilerParams(vmem_limit_bytes=8 * 1024 * 1024),
        name="finish",
    )(ready, scale, router)


def solution(mesh):
    return jax.shard_map(
        functools.partial(on_device, mesh.shape["rows"], mesh.shape["owner"]),
        mesh=mesh,
        in_specs=(
            P("owner", "rows", None),
            P("owner", "rows", None),
            P("rows", "owner"),
            P("rows"),
        ),
        out_specs=(
            P(("owner", "rows"), None, None),
            P(("owner", "rows"), None, None),
            P(("owner", "rows"), None),
            P(("owner", "rows"), None),
            P(),
        ),
        check_vma=False,
    )
```

```python
import functools

import jax
import jax.numpy as jnp
from jax import lax
from jax.experimental import pallas as pl
from jax.experimental.pallas import tpu as pltpu
from jax.sharding import PartitionSpec as P

MESH = pl.DeviceIdType.MESH
CHUNK = 32
RING = 10
PARTS = 4


def split(n):
    return max(d for d in range(1, n + 1) if d * d <= n and n % d == 0)


def across_first(n):
    if n == 1:
        return []
    half = n // 2
    return list(range(half, n)) + across_first(half)


def partner(at, k):
    other, bit = at, 1
    while bit <= k:
        if k & bit:
            other = other + bit * (1 - 2 * ((at // bit) % 2))
        bit *= 2
    return other


def routes(n, me):
    wide = split(n)
    deep = n // wide
    z, y = me // wide, lax.rem(me, wide)
    place, groups = [me], []
    for far in across_first(deep) + [0]:
        group = []
        for near in range(wide):
            if far or near:
                group.append(len(place))
                place.append(partner(z, far) * wide + partner(y, near))
        groups.append(group)
    return wide, place, groups


def kernel(
    rows_n, owners_n,
    gate, up, weight, gain,
    ready, scale, router,
    slabs, send, part, gathered, relayed, halves, other, first, first_by, scales, mine,
    load_sem, data_send, data_recv, first_send, first_recv,
    relay_send, relay_recv, cross_send, cross_recv, spread_send, spread_recv,
    router_send, router_recv, forward_send, forward_recv,
):
    me, group = lax.axis_index("rows"), lax.axis_index("owner")
    height, width = gate.shape[2], gate.shape[3]
    each = gate.shape[1]
    steps = 2 * each
    wide, place, groups = routes(rows_n, me)
    half = rows_n // 2
    close = [k for lot in groups[half // wide :] for k in lot]
    mate, side = place[1], (me // half) * half
    peers = list(range(1, rows_n))
    order = peers + [0]
    here = pl.ds(pl.multiple_of(me * height, height), height)

    pieces = [(step, k) for step in range(1, steps) for k in order]
    turns = pieces + pieces

    def load(slot, step, k):
        bank, c = (gate, up)[step // each], step % each
        return pltpu.make_async_copy(bank.at[place[k], c], slabs.at[slot], load_sem.at[slot])

    def turn_copy(t):
        return load(rows_n + t % RING, *turns[t])

    def begin(copies):
        for copy in copies:
            copy.start()

    def sum_one(slot, k, step):
        def add(i, total):
            x = slabs[slot, pl.ds(i * CHUNK, CHUNK), :]
            return total + jnp.sum((x * x).reshape(CHUNK // 8, 8, width), axis=0)

        total = lax.fori_loop(0, height // CHUNK, add, jnp.zeros((8, width), jnp.float32))
        part[place[k], step] = jnp.sum(total, axis=0, keepdims=True)

    def to_peer(source, target, out_sem, in_sem, k):
        return pltpu.make_async_remote_copy(
            source, target, out_sem, in_sem, device_id={"rows": place[k]}, device_id_type=MESH
        )

    def ahead(device):
        return pl.ds(partner(device // wide, half // wide) * wide, wide)

    def first_copies(arriving=False):
        return [
            to_peer(
                part.at[ahead(place[k]), 0], first.at[me],
                first_send.at[k], first_recv.at[place[k] if arriving else me], k,
            )
            for k in peers
        ]

    lots = [(0, 2)] + ([(2, steps - 2)] if steps > 2 else [])

    def relay_copies(lot, arriving=False):
        span = pl.ds(*lots[lot])
        return [
            to_peer(
                part.at[device, span], bank.at[me, span],
                relay_send.at[lot, which, k],
                relay_recv.at[lot, which, place[k] if arriving else me], k,
            )
            for k in close
            for which, (bank, device) in enumerate(
                ((gathered, place[k]), (relayed, partner(place[k] // wide, half // wide) * wide + lax.rem(place[k], wide)))
            )
        ]

    def cross_copy(lot):
        span = pl.ds(*lots[lot])
        return to_peer(
            halves.at[pl.ds(0, 2), span], other.at[pl.ds(0, 2), span],
            cross_send.at[lot], cross_recv.at[lot], 1,
        )

    def spread_copies(lot, arriving=False):
        span = pl.ds(*lots[lot])
        return [
            to_peer(
                scales.at[device, span], scales.at[device, span],
                spread_send.at[lot, which, k],
                spread_recv.at[lot, which, place[k] if arriving else me], k,
            )
            for k in close
            for which, device in enumerate((me, mate))
        ]

    def arrive(copies):
        for copy in copies:
            copy.wait_recv()

    def finish_first():
        first[me] = part[ahead(me), 0]
        total = [first[0], first[half]]
        for i in range(1, half):
            total = [total[0] + first[i], total[1] + first[half + i]]
        first_by[...] = jnp.sqrt(total[0] + total[1])

    def halve(lot):
        span = pl.ds(*lots[lot])
        gathered[me, span] = part[me, span]
        relayed[me, span] = part[mate, span]
        for which, bank in enumerate((gathered, relayed)):
            total = bank[side, span]
            for i in range(1, half):
                total = total + bank[side + i, span]
            halves[which, span] = total

    def finish_lot(lot):
        span = pl.ds(*lots[lot])
        root = jnp.sqrt(halves[0, span] + other[1, span])
        scales[me, span] = root
        scale[span] = root
        scales[mate, span] = jnp.sqrt(halves[1, span] + other[0, span])

    def data_copy(step, k, arriving=False):
        return pltpu.make_async_remote_copy(
            send.at[step, k - 1], ready.at[step, here],
            data_send.at[step, k], data_recv.at[step, place[k] if arriving else me],
            device_id={"rows": place[k]}, device_id_type=MESH,
        )

    def narrow(slot, k, step):
        by = scales[place[k], step]

        def one(i, carry):
            at = pl.ds(i * CHUNK, CHUNK)
            ready_rows = pl.ds(pl.multiple_of(me * height + i * CHUNK, CHUNK), CHUNK)
            value = (slabs[slot, at, :] / by).astype(jnp.bfloat16)
            if k == 0:
                ready[step, ready_rows, :] = value
            else:
                send[step, k - 1, at, :] = value
            return carry

        lax.fori_loop(0, height // CHUNK, one, 0)
        if k in groups[0] and step > 1:
            data_copy(step, k).start()

    tall = height // PARTS

    def cover(step, turn):
        k, piece = turn % wide + 1, turn // wide
        at = pl.ds(piece * tall, tall)
        if step == 0:
            by = first_by[lax.rem(place[k], wide)]
            send[0, k - 1, at, :] = (slabs[k, at, :] / by).astype(jnp.bfloat16)
        to_peer(
            send.at[step, k - 1, at],
            ready.at[step, pl.ds(pl.multiple_of(me * height + piece * tall, tall), tall)],
            data_send.at[step, k], data_recv.at[step, me], k,
        ).start()

    def send_group(lot, step):
        for k in lot:
            data_copy(step, k).start()

    for k in order:
        load(k, 0, k).start()

    barrier = pltpu.get_barrier_semaphore()
    for k in peers:
        pl.semaphore_signal(barrier, inc=1, device_id={"rows": place[k]}, device_id_type=MESH)
    for j in range(1, owners_n):
        pl.semaphore_signal(
            barrier, inc=1, device_id={"owner": lax.rem(group + j, owners_n)}, device_id_type=MESH
        )

    columns = pl.ds(pl.multiple_of(me * height, height), height)
    mine[...] = (weight[...] * gain[...]).astype(jnp.bfloat16)
    router[group, :, columns] = mine[...]

    def router_copies(arriving=False):
        return [
            to_peer(
                mine, router.at[group, :, columns],
                router_send.at[k], router_recv.at[place[k] if arriving else me], k,
            )
            for k in peers
        ]

    pl.semaphore_wait(barrier, rows_n + owners_n - 2)

    for k in order:
        load(k, 0, k).wait()
        sum_one(k, k, 0)
    first_out = first_copies()
    begin(first_out)
    router_out = router_copies()
    begin(router_out)
    for t in range(RING):
        turn_copy(t).start()
    arrive(first_copies(True))
    finish_first()
    covers = list(range(PARTS * wide))
    quarter = len(covers) // 4
    for turn in covers[:quarter]:
        cover(0, turn)

    def take(t, use):
        step, k = turns[t]
        turn_copy(t).wait()
        use(rows_n + t % RING, k, step)
        if t + RING < len(turns):
            turn_copy(t + RING).start()

    def take_steps(base, lo, hi, use):
        for t in range(base + (lo - 1) * rows_n, base + (hi - 1) * rows_n):
            take(t, use)

    third = (steps - 2) // 3
    batches = range(len(lots))
    relay_out = [relay_copies(lot) for lot in batches]
    cross = [cross_copy(lot) for lot in batches]
    spread_out = [spread_copies(lot) for lot in batches]

    take_steps(0, 1, 2, sum_one)
    begin(relay_out[0])
    for turn in covers[quarter : 2 * quarter]:
        cover(0, turn)
    take_steps(0, 2, 2 + third, sum_one)
    arrive(relay_copies(0, True))
    halve(0)
    cross[0].start()
    for turn in covers[2 * quarter : 3 * quarter]:
        cover(0, turn)
    take_steps(0, 2 + third, 2 + 2 * third, sum_one)
    cross[0].wait_recv()
    finish_lot(0)
    begin(spread_out[0])
    for turn in covers[3 * quarter :]:
        cover(0, turn)
    take_steps(0, 2 + 2 * third, steps, sum_one)
    for copies in relay_out[1:]:
        begin(copies)
    arrive(spread_copies(0, True))
    base = len(pieces)
    for k in groups[0]:
        take(base + k - 1, narrow)
    for turn in covers[:quarter]:
        cover(1, turn)
    for lot in batches[1:]:
        arrive(relay_copies(lot, True))
        halve(lot)
        cross[lot].start()
    for turn in covers[quarter : 2 * quarter]:
        cover(1, turn)
    for lot in batches[1:]:
        cross[lot].wait_recv()
        finish_lot(lot)
        begin(spread_out[lot])
    for turn in covers[2 * quarter :]:
        cover(1, turn)
    for t in range(base + len(groups[0]), base + rows_n):
        take(t, narrow)
    for lot in batches[1:]:
        arrive(spread_copies(lot, True))

    take_steps(base, 2, steps, narrow)
    for k in order:
        if k not in groups[0]:
            narrow(k, k, 0)
    for lot in groups[1:]:
        for step in range(steps):
            send_group(lot, step)

    arrive(router_copies(True))
    forwards = []
    for j in range(1, owners_n):
        forwards.append(
            pltpu.make_async_remote_copy(
                router.at[group], router.at[group], forward_send.at[j], forward_recv.at[j],
                device_id={"owner": lax.rem(group + j, owners_n)}, device_id_type=MESH,
            )
        )
    begin(forwards)

    for copy in cross:
        copy.wait_send()
    for copies in (first_out, *relay_out, *spread_out, router_out):
        for copy in copies:
            copy.wait_send()
    for copy in forwards:
        copy.wait()
    for step in range(steps):
        for k in peers:
            data_copy(step, k).wait_send()
            data_copy(step, k, True).wait_recv()


def finish(
    each, ready, scale, router,
    ready_gate, ready_up, scale_gate, scale_up, serve_router,
    low, high, turned, sem, small_sem,
):
    banks = ready_gate, ready_up
    copies = [
        pltpu.make_async_copy(ready.at[step], banks[step // each].at[step % each], sem.at[step])
        for step in range(2 * each)
    ]
    for copy in copies:
        copy.start()
    low[...] = scale[pl.ds(0, each)].reshape(low.shape)
    high[...] = scale[pl.ds(each, each)].reshape(high.shape)
    owners, cols, rows = router.shape
    turned[...] = router[...].reshape(owners * cols, rows).T
    small = [
        pltpu.make_async_copy(source, target, small_sem.at[i])
        for i, (source, target) in enumerate(
            ((low, scale_gate), (high, scale_up), (turned, serve_router))
        )
    ]
    for copy in small:
        copy.start()
    for copy in copies + small:
        copy.wait()


def on_device(rows_n, owners_n, train_gate, train_up, router_weight, router_gain):
    experts, height, width = train_gate.shape
    each = experts // rows_n
    steps = 2 * each
    cols = router_weight.shape[1]
    f32, bf16, dma = jnp.float32, jnp.bfloat16, pltpu.SemaphoreType.DMA
    hbm, vmem = pl.BlockSpec(memory_space=pl.ANY), pl.BlockSpec(memory_space=pltpu.VMEM)
    landing = 2 * steps * rows_n * height * width
    ready, scale, router = pl.pallas_call(
        functools.partial(kernel, rows_n, owners_n),
        out_shape=(
            pltpu.VMEM((steps, rows_n * height, width), bf16),
            pltpu.VMEM((steps, 1, width), f32),
            pltpu.VMEM((owners_n, cols, rows_n * height), bf16),
        ),
        in_specs=[hbm, hbm, vmem, vmem],
        out_specs=(vmem, vmem, vmem),
        scratch_shapes=[
            pltpu.VMEM((rows_n + RING, height, width), f32),
            pltpu.VMEM((steps, rows_n - 1, height, width), bf16),
            pltpu.VMEM((rows_n, steps, 1, width), f32),
            pltpu.VMEM((rows_n, steps, 1, width), f32),
            pltpu.VMEM((rows_n, steps, 1, width), f32),
            pltpu.VMEM((2, steps, 1, width), f32),
            pltpu.VMEM((2, steps, 1, width), f32),
            pltpu.VMEM((rows_n, split(rows_n), 1, width), f32),
            pltpu.VMEM((split(rows_n), 1, width), f32),
            pltpu.VMEM((rows_n, steps, 1, width), f32),
            pltpu.VMEM((cols, height), bf16),
            dma((rows_n + RING,)),
            dma((steps, rows_n)),
            dma((steps, rows_n)),
            dma((rows_n,)),
            dma((rows_n,)),
            dma((2, 2, rows_n)),
            dma((2, 2, rows_n)),
            dma((2,)),
            dma((2,)),
            dma((2, 2, rows_n)),
            dma((2, 2, rows_n)),
            dma((rows_n,)),
            dma((rows_n,)),
            dma((owners_n,)),
            dma((owners_n,)),
        ],
        compiler_params=pltpu.CompilerParams(
            collective_id=0, has_side_effects=True, vmem_limit_bytes=61 * 1024 * 1024 - landing
        ),
        name="serve",
    )(
        train_gate.reshape(rows_n, each, height, width),
        train_up.reshape(rows_n, each, height, width),
        router_weight.T,
        router_gain[None, :],
    )
    bank = jax.ShapeDtypeStruct((each, rows_n * height, width), bf16)
    scales = jax.ShapeDtypeStruct((each, width), f32)
    return pl.pallas_call(
        functools.partial(finish, each),
        out_shape=(bank, bank, scales, scales, jax.ShapeDtypeStruct((rows_n * height, owners_n * cols), bf16)),
        in_specs=[vmem, vmem, vmem],
        out_specs=(hbm, hbm, hbm, hbm, hbm),
        scratch_shapes=[
            pltpu.VMEM((each, width), f32),
            pltpu.VMEM((each, width), f32),
            pltpu.VMEM((rows_n * height, owners_n * cols), bf16),
            dma((steps,)),
            dma((3,)),
        ],
        compiler_params=pltpu.CompilerParams(vmem_limit_bytes=8 * 1024 * 1024),
        name="finish",
    )(ready, scale, router)


def solution(mesh):
    return jax.shard_map(
        functools.partial(on_device, mesh.shape["rows"], mesh.shape["owner"]),
        mesh=mesh,
        in_specs=(
            P("owner", "rows", None),
            P("owner", "rows", None),
            P("rows", "owner"),
            P("rows"),
        ),
        out_specs=(
            P(("owner", "rows"), None, None),
            P(("owner", "rows"), None, None),
            P(("owner", "rows"), None),
            P(("owner", "rows"), None),
            P(),
        ),
        check_vma=False,
    )
```

```python
import functools

import jax
import jax.numpy as jnp
from jax import lax
from jax.experimental import pallas as pl
from jax.experimental.pallas import tpu as pltpu
from jax.sharding import PartitionSpec as P

MESH = pl.DeviceIdType.MESH
CHUNK = 32
RING = 10
PARTS = 4


def split(n):
    return max(d for d in range(1, n + 1) if d * d <= n and n % d == 0)


def across_first(n):
    if n == 1:
        return []
    half = n // 2
    return list(range(half, n)) + across_first(half)


def partner(at, k):
    other, bit = at, 1
    while bit <= k:
        if k & bit:
            other = other + bit * (1 - 2 * ((at // bit) % 2))
        bit *= 2
    return other


def routes(n, me):
    wide = split(n)
    deep = n // wide
    z, y = me // wide, lax.rem(me, wide)
    place, groups = [me], []
    for far in across_first(deep) + [0]:
        group = []
        for near in range(wide):
            if far or near:
                group.append(len(place))
                place.append(partner(z, far) * wide + partner(y, near))
        groups.append(group)
    return wide, place, groups


def kernel(
    rows_n, owners_n,
    gate, up, weight, gain,
    ready, scale, router,
    slabs, send, part, gathered, relayed, halves, other, first, first_by, scales, mine,
    weight_in, gain_in, small_sem,
    load_sem, data_send, data_recv, first_send, first_recv,
    relay_send, relay_recv, cross_send, cross_recv, spread_send, spread_recv,
    router_send, router_recv, forward_send, forward_recv,
):
    me, group = lax.axis_index("rows"), lax.axis_index("owner")
    height, width = gate.shape[2], gate.shape[3]
    each = gate.shape[1]
    steps = 2 * each
    wide, place, groups = routes(rows_n, me)
    half = rows_n // 2
    close = [k for lot in groups[half // wide :] for k in lot]
    mate, side = place[1], (me // half) * half
    peers = list(range(1, rows_n))
    order = peers + [0]
    here = pl.ds(pl.multiple_of(me * height, height), height)

    pieces = [(step, k) for step in range(1, steps) for k in order]
    turns = pieces + pieces

    def load(slot, step, k):
        bank, c = (gate, up)[step // each], step % each
        return pltpu.make_async_copy(bank.at[place[k], c], slabs.at[slot], load_sem.at[slot])

    def turn_copy(t):
        return load(rows_n + t % RING, *turns[t])

    def begin(copies):
        for copy in copies:
            copy.start()

    def sum_one(slot, k, step):
        def add(i, total):
            x = slabs[slot, pl.ds(i * CHUNK, CHUNK), :]
            return total + jnp.sum((x * x).reshape(CHUNK // 8, 8, width), axis=0)

        total = lax.fori_loop(0, height // CHUNK, add, jnp.zeros((8, width), jnp.float32))
        part[place[k], step] = jnp.sum(total, axis=0, keepdims=True)

    def to_peer(source, target, out_sem, in_sem, k):
        return pltpu.make_async_remote_copy(
            source, target, out_sem, in_sem, device_id={"rows": place[k]}, device_id_type=MESH
        )

    def ahead(device):
        return pl.ds(partner(device // wide, half // wide) * wide, wide)

    def first_copies(arriving=False):
        return [
            to_peer(
                part.at[ahead(place[k]), 0], first.at[me],
                first_send.at[k], first_recv.at[place[k] if arriving else me], k,
            )
            for k in peers
        ]

    lots = [(0, 2)] + ([(2, steps - 2)] if steps > 2 else [])

    def relay_copies(lot, arriving=False):
        span = pl.ds(*lots[lot])
        return [
            to_peer(
                part.at[device, span], bank.at[me, span],
                relay_send.at[lot, which, k],
                relay_recv.at[lot, which, place[k] if arriving else me], k,
            )
            for k in close
            for which, (bank, device) in enumerate(
                ((gathered, place[k]), (relayed, partner(place[k] // wide, half // wide) * wide + lax.rem(place[k], wide)))
            )
        ]

    def cross_copy(lot):
        span = pl.ds(*lots[lot])
        return to_peer(
            halves.at[pl.ds(0, 2), span], other.at[pl.ds(0, 2), span],
            cross_send.at[lot], cross_recv.at[lot], 1,
        )

    def spread_copies(lot, arriving=False):
        span = pl.ds(*lots[lot])
        return [
            to_peer(
                scales.at[device, span], scales.at[device, span],
                spread_send.at[lot, which, k],
                spread_recv.at[lot, which, place[k] if arriving else me], k,
            )
            for k in close
            for which, device in enumerate((me, mate))
        ]

    def arrive(copies):
        for copy in copies:
            copy.wait_recv()

    def finish_first():
        first[me] = part[ahead(me), 0]
        total = [first[0], first[half]]
        for i in range(1, half):
            total = [total[0] + first[i], total[1] + first[half + i]]
        first_by[...] = jnp.sqrt(total[0] + total[1])

    def halve(lot):
        span = pl.ds(*lots[lot])
        gathered[me, span] = part[me, span]
        relayed[me, span] = part[mate, span]
        for which, bank in enumerate((gathered, relayed)):
            total = bank[side, span]
            for i in range(1, half):
                total = total + bank[side + i, span]
            halves[which, span] = total

    def finish_lot(lot):
        span = pl.ds(*lots[lot])
        root = jnp.sqrt(halves[0, span] + other[1, span])
        scales[me, span] = root
        scale[span] = root
        scales[mate, span] = jnp.sqrt(halves[1, span] + other[0, span])

    def data_copy(step, k, arriving=False):
        return pltpu.make_async_remote_copy(
            send.at[step, k - 1], ready.at[step, here],
            data_send.at[step, k], data_recv.at[step, place[k] if arriving else me],
            device_id={"rows": place[k]}, device_id_type=MESH,
        )

    def narrow(slot, k, step):
        by = scales[place[k], step]

        def one(i, carry):
            at = pl.ds(i * CHUNK, CHUNK)
            ready_rows = pl.ds(pl.multiple_of(me * height + i * CHUNK, CHUNK), CHUNK)
            value = (slabs[slot, at, :] / by).astype(jnp.bfloat16)
            if k == 0:
                ready[step, ready_rows, :] = value
            else:
                send[step, k - 1, at, :] = value
            return carry

        lax.fori_loop(0, height // CHUNK, one, 0)
        if k in groups[0] and step > 1:
            data_copy(step, k).start()

    tall = height // PARTS

    def cover(step, turn):
        k, piece = turn % wide + 1, turn // wide
        at = pl.ds(piece * tall, tall)
        if step == 0:
            by = first_by[lax.rem(place[k], wide)]
            send[0, k - 1, at, :] = (slabs[k, at, :] / by).astype(jnp.bfloat16)
        to_peer(
            send.at[step, k - 1, at],
            ready.at[step, pl.ds(pl.multiple_of(me * height + piece * tall, tall), tall)],
            data_send.at[step, k], data_recv.at[step, me], k,
        ).start()

    def send_group(lot, step):
        for k in lot:
            data_copy(step, k).start()

    for k in order:
        load(k, 0, k).start()

    barrier = pltpu.get_barrier_semaphore()
    for k in peers:
        pl.semaphore_signal(barrier, inc=1, device_id={"rows": place[k]}, device_id_type=MESH)
    for j in range(1, owners_n):
        pl.semaphore_signal(
            barrier, inc=1, device_id={"owner": lax.rem(group + j, owners_n)}, device_id_type=MESH
        )

    columns = pl.ds(pl.multiple_of(me * height, height), height)
    small_in = [
        pltpu.make_async_copy(weight, weight_in, small_sem.at[0]),
        pltpu.make_async_copy(gain, gain_in, small_sem.at[1]),
    ]
    begin(small_in)

    def router_copies(arriving=False):
        return [
            to_peer(
                mine, router.at[group, :, columns],
                router_send.at[k], router_recv.at[place[k] if arriving else me], k,
            )
            for k in peers
        ]


    for k in order:
        load(k, 0, k).wait()
        sum_one(k, k, 0)
    first_out = first_copies()
    pl.semaphore_wait(barrier, rows_n + owners_n - 2)
    begin(first_out)
    arrive(small_in)
    mine[...] = (weight_in[...] * gain_in[...]).astype(jnp.bfloat16)
    router[group, :, columns] = mine[...]
    router_out = router_copies()
    begin(router_out)
    for t in range(RING):
        turn_copy(t).start()
    arrive(first_copies(True))
    finish_first()
    covers = list(range(PARTS * wide))
    quarter = len(covers) // 4
    for turn in covers[:quarter]:
        cover(0, turn)

    def take(t, use):
        step, k = turns[t]
        turn_copy(t).wait()
        use(rows_n + t % RING, k, step)
        if t + RING < len(turns):
            turn_copy(t + RING).start()

    def take_steps(base, lo, hi, use):
        for t in range(base + (lo - 1) * rows_n, base + (hi - 1) * rows_n):
            take(t, use)

    third = (steps - 2) // 3
    batches = range(len(lots))
    relay_out = [relay_copies(lot) for lot in batches]
    cross = [cross_copy(lot) for lot in batches]
    spread_out = [spread_copies(lot) for lot in batches]

    take_steps(0, 1, 2, sum_one)
    begin(relay_out[0])
    for turn in covers[quarter : 2 * quarter]:
        cover(0, turn)
    take_steps(0, 2, 2 + third, sum_one)
    arrive(relay_copies(0, True))
    halve(0)
    cross[0].start()
    for turn in covers[2 * quarter : 3 * quarter]:
        cover(0, turn)
    take_steps(0, 2 + third, 2 + 2 * third, sum_one)
    cross[0].wait_recv()
    finish_lot(0)
    begin(spread_out[0])
    for turn in covers[3 * quarter :]:
        cover(0, turn)
    take_steps(0, 2 + 2 * third, steps, sum_one)
    for copies in relay_out[1:]:
        begin(copies)
    arrive(spread_copies(0, True))
    base = len(pieces)
    for k in groups[0]:
        take(base + k - 1, narrow)
    for turn in covers[:quarter]:
        cover(1, turn)
    for lot in batches[1:]:
        arrive(relay_copies(lot, True))
        halve(lot)
        cross[lot].start()
    for turn in covers[quarter : 2 * quarter]:
        cover(1, turn)
    for lot in batches[1:]:
        cross[lot].wait_recv()
        finish_lot(lot)
        begin(spread_out[lot])
    for turn in covers[2 * quarter :]:
        cover(1, turn)
    for t in range(base + len(groups[0]), base + rows_n):
        take(t, narrow)
    for lot in batches[1:]:
        arrive(spread_copies(lot, True))

    take_steps(base, 2, steps, narrow)
    for k in order:
        if k not in groups[0]:
            narrow(k, k, 0)
    for lot in groups[1:]:
        for step in range(steps):
            send_group(lot, step)

    arrive(router_copies(True))
    forwards = []
    for j in range(1, owners_n):
        forwards.append(
            pltpu.make_async_remote_copy(
                router.at[group], router.at[group], forward_send.at[j], forward_recv.at[j],
                device_id={"owner": lax.rem(group + j, owners_n)}, device_id_type=MESH,
            )
        )
    begin(forwards)

    for copy in cross:
        copy.wait_send()
    for copies in (first_out, *relay_out, *spread_out, router_out):
        for copy in copies:
            copy.wait_send()
    for copy in forwards:
        copy.wait()
    for step in range(steps):
        for k in peers:
            data_copy(step, k).wait_send()
            data_copy(step, k, True).wait_recv()


def finish(
    each, ready, scale, router,
    ready_gate, ready_up, scale_gate, scale_up, serve_router,
    low, high, turned, sem, small_sem,
):
    banks = ready_gate, ready_up
    copies = [
        pltpu.make_async_copy(ready.at[step], banks[step // each].at[step % each], sem.at[step])
        for step in range(2 * each)
    ]
    for copy in copies:
        copy.start()
    low[...] = scale[pl.ds(0, each)].reshape(low.shape)
    high[...] = scale[pl.ds(each, each)].reshape(high.shape)
    owners, cols, rows = router.shape
    turned[...] = router[...].reshape(owners * cols, rows).T
    small = [
        pltpu.make_async_copy(source, target, small_sem.at[i])
        for i, (source, target) in enumerate(
            ((low, scale_gate), (high, scale_up), (turned, serve_router))
        )
    ]
    for copy in small:
        copy.start()
    for copy in copies + small:
        copy.wait()


def on_device(rows_n, owners_n, train_gate, train_up, router_weight, router_gain):
    experts, height, width = train_gate.shape
    each = experts // rows_n
    steps = 2 * each
    cols = router_weight.shape[1]
    f32, bf16, dma = jnp.float32, jnp.bfloat16, pltpu.SemaphoreType.DMA
    hbm, vmem = pl.BlockSpec(memory_space=pl.ANY), pl.BlockSpec(memory_space=pltpu.VMEM)
    landing = 2 * steps * rows_n * height * width
    ready, scale, router = pl.pallas_call(
        functools.partial(kernel, rows_n, owners_n),
        out_shape=(
            pltpu.VMEM((steps, rows_n * height, width), bf16),
            pltpu.VMEM((steps, 1, width), f32),
            pltpu.VMEM((owners_n, cols, rows_n * height), bf16),
        ),
        in_specs=[hbm, hbm, hbm, hbm],
        out_specs=(vmem, vmem, vmem),
        scratch_shapes=[
            pltpu.VMEM((rows_n + RING, height, width), f32),
            pltpu.VMEM((steps, rows_n - 1, height, width), bf16),
            pltpu.VMEM((rows_n, steps, 1, width), f32),
            pltpu.VMEM((rows_n, steps, 1, width), f32),
            pltpu.VMEM((rows_n, steps, 1, width), f32),
            pltpu.VMEM((2, steps, 1, width), f32),
            pltpu.VMEM((2, steps, 1, width), f32),
            pltpu.VMEM((rows_n, split(rows_n), 1, width), f32),
            pltpu.VMEM((split(rows_n), 1, width), f32),
            pltpu.VMEM((rows_n, steps, 1, width), f32),
            pltpu.VMEM((cols, height), bf16),
            pltpu.VMEM((cols, height), f32),
            pltpu.VMEM((1, height), f32),
            dma((2,)),
            dma((rows_n + RING,)),
            dma((steps, rows_n)),
            dma((steps, rows_n)),
            dma((rows_n,)),
            dma((rows_n,)),
            dma((2, 2, rows_n)),
            dma((2, 2, rows_n)),
            dma((2,)),
            dma((2,)),
            dma((2, 2, rows_n)),
            dma((2, 2, rows_n)),
            dma((rows_n,)),
            dma((rows_n,)),
            dma((owners_n,)),
            dma((owners_n,)),
        ],
        compiler_params=pltpu.CompilerParams(
            collective_id=0, has_side_effects=True, vmem_limit_bytes=61 * 1024 * 1024 - landing
        ),
        name="serve",
    )(
        train_gate.reshape(rows_n, each, height, width),
        train_up.reshape(rows_n, each, height, width),
        router_weight.T,
        router_gain[None, :],
    )
    bank = jax.ShapeDtypeStruct((each, rows_n * height, width), bf16)
    scales = jax.ShapeDtypeStruct((each, width), f32)
    return pl.pallas_call(
        functools.partial(finish, each),
        out_shape=(bank, bank, scales, scales, jax.ShapeDtypeStruct((rows_n * height, owners_n * cols), bf16)),
        in_specs=[vmem, vmem, vmem],
        out_specs=(hbm, hbm, hbm, hbm, hbm),
        scratch_shapes=[
            pltpu.VMEM((each, width), f32),
            pltpu.VMEM((each, width), f32),
            pltpu.VMEM((rows_n * height, owners_n * cols), bf16),
            dma((steps,)),
            dma((3,)),
        ],
        compiler_params=pltpu.CompilerParams(vmem_limit_bytes=8 * 1024 * 1024),
        name="finish",
    )(ready, scale, router)


def solution(mesh):
    return jax.shard_map(
        functools.partial(on_device, mesh.shape["rows"], mesh.shape["owner"]),
        mesh=mesh,
        in_specs=(
            P("owner", "rows", None),
            P("owner", "rows", None),
            P("rows", "owner"),
            P("rows"),
        ),
        out_specs=(
            P(("owner", "rows"), None, None),
            P(("owner", "rows"), None, None),
            P(("owner", "rows"), None),
            P(("owner", "rows"), None),
            P(),
        ),
        check_vma=False,
    )
```
